32 devices in a mesh: snap: 8 (over z, x), bin: 4 (over y, core).
Axes of the slice: x: 2, y: 2, z: 4, core: 2. Of those that a mesh axis runs over, the one named last changes fastest.
Arguments:
- data: bfloat16 [256, 128, 1024], P(None, ('snap', 'bin')), may hold values from -6 to 6
- steering: bfloat16 [256, 1024, 2048], P(('snap', 'bin')), may hold values from -2 to 2
- start: float32 [256, 1024, 64], P(('snap', 'bin')), may hold values from -6 to 6
Outputs:
- projector: float32 [256, 1024, 1024], P(('snap', 'bin'))
- spectrum: float32 [2048], replicated
The draws below stay inside these ranges and needn't reach their ends.
All inputs are finite; a program needn't handle non-finite values.
Results may differ from the reference program's by a relative error of at most 0.00042.
Values may be sent and summed in bfloat16 or wider, within the bound.
A program may use at most 128 MiB of HBM per device.

```python
import math
import jax
import jax.numpy as jnp
from jax import lax

M = 1024
F = 256
SOURCES = 64
G = 2048
ITERS = 3
K2 = 128


def array_pieces(key):
    sines = jax.random.uniform(jax.random.fold_in(key, 101), (G,), jnp.float32, -1.0, 1.0)
    fraction = jax.random.uniform(jax.random.fold_in(key, 102), (F,), jnp.float32, 0.5, 1.0)
    gains = jnp.exp(jax.random.uniform(jax.random.fold_in(key, 103), (F, M), jnp.float32, -0.34, 0.34))
    return (sines, fraction, gains)


def steer_columns(fraction, gains, sines):
    half = M // 2
    places = jnp.arange(half, dtype=jnp.float32) - (half - 1) / 2.0
    phase = jnp.pi * fraction * places[:, None] * sines[None, :]
    table = jnp.concatenate([jnp.cos(phase), jnp.sin(phase)], axis=0) * 1.4142135
    return table * gains[:, None]


def draw_steering(key, part):
    sines, fraction, gains = array_pieces(key)

    def one_table(items):
        return steer_columns(items[0], items[1], sines).astype(jnp.bfloat16)
    return lax.map(one_table, (fraction, gains))


def draw_data(key, part):
    sines, fraction, gains = array_pieces(key)
    chosen = jax.random.permutation(jax.random.fold_in(key, 104), G)[:SOURCES]
    picked = jnp.take(sines, chosen)
    bulk_edge = (1.0 + (M / K2) ** 0.5) ** 2
    ratio = jnp.exp(jax.random.uniform(jax.random.fold_in(key, 105), (F, SOURCES), jnp.float32, math.log(2.5), math.log(10.0)))
    levels = jnp.sqrt(bulk_edge * ratio / M)
    bin_keys = jax.random.split(jax.random.fold_in(key, 106), F)

    def one_bin(items):
        frac, gain, level, sub_key = items
        columns = steer_columns(frac, gain, picked)
        amp_key = jax.random.fold_in(sub_key, 1)
        noise_key = jax.random.fold_in(sub_key, 2)
        amps = jax.random.truncated_normal(amp_key, -4.0, 4.0, (K2, SOURCES), jnp.float32)
        noise = jax.random.truncated_normal(noise_key, -4.0, 4.0, (K2, M), jnp.float32)
        signal = jnp.dot(amps * level[None, :], columns.T, precision=lax.Precision.HIGHEST)
        return jnp.clip(signal + noise, -6.0, 6.0).astype(jnp.bfloat16)
    return lax.map(one_bin, (fraction, gains, levels, bin_keys))


def shard_levels(key, shape, cuts, least, high):
    def one(axis_at, blocks):
        steps = jax.random.uniform(jax.random.fold_in(jax.random.fold_in(key, 6), axis_at), (blocks,), jnp.float32, least / len(cuts), high / len(cuts))
        return jnp.repeat(jnp.exp(steps), shape[axis_at] // blocks).reshape((-1,) + (1,) * (len(shape) - axis_at - 1))

    factor_of = one(*cuts[0])
    for cut in cuts[1:]:
        factor_of = factor_of * one(*cut)
    return factor_of


def bell_draw(key, extent, width, reach, pieces=(), held_as=jnp.bfloat16):
    level = shard_levels(key, extent, pieces, -0.22, 0.18) if pieces else 1.0
    values = jax.random.normal(key, extent, jnp.float32) * width * level
    return jnp.minimum(jnp.maximum(values, -reach), reach).astype(held_as)


def setup_inputs(seed: int = 0) -> dict:
    seeds = jax.random.split(jax.random.key(seed), 4)
    data = draw_data(jax.random.fold_in(seeds[3], 71), 0)
    steering = draw_steering(jax.random.fold_in(seeds[3], 71), 0)
    start = bell_draw(seeds[2], (F, M, SOURCES), 1.0, 6.0, ((0, 32),), jnp.float32)
    return {"data": data, "steering": steering, "start": start}


def one_bin(snaps, steer, basis):
    covar = jnp.dot(snaps.T.astype(jnp.float32), snaps.astype(jnp.float32), preferred_element_type=jnp.float32) / snaps.shape[0]
    for step in range(ITERS):
        image = jnp.dot(covar, basis, precision=lax.Precision.HIGHEST)
        gram_mat = jnp.dot(image.T, image, precision=lax.Precision.HIGHEST)
        lower_factor = jnp.linalg.cholesky(gram_mat)
        basis = jax.scipy.linalg.solve_triangular(lower_factor, image.T, lower=True).T
    projector = jnp.dot(basis, basis.T, precision=lax.Precision.HIGHEST)
    basis_low = basis.astype(jnp.bfloat16)
    along = jnp.dot(basis_low.T.astype(jnp.float32), steer.astype(jnp.float32), preferred_element_type=jnp.float32)
    steer_wide = steer.astype(jnp.float32)
    energy = jnp.sum(steer_wide * steer_wide, axis=0)
    noise = energy - jnp.sum(along * along, axis=0)
    return (projector, noise)

def reference(data, steering, start):
    projector, noise = lax.map(lambda items: one_bin(items[0], items[1], items[2]), (data, steering, start))
    spectrum = F * M / jnp.sum(noise, axis=0)
    return (projector, spectrum)
```

```python
import functools

import jax
import jax.numpy as jnp
from jax import lax
from jax.experimental import pallas as pl
from jax.experimental.pallas import tpu as pltpu

ITERS = 3
F32 = jnp.float32
BF16 = jnp.bfloat16
MESH = pl.DeviceIdType.MESH
VMEM_LIMIT = 60 * 1024 * 1024
BOTH = ("snap", "bin")


def place(d, inner):
    return (d // inner, lax.rem(d, inner))


def greet_all(me, n, inner):
    barrier = pltpu.get_barrier_semaphore()

    def one(o, c):
        pl.semaphore_signal(
            barrier, inc=1, device_id=place(lax.rem(me + o, n), inner), device_id_type=MESH
        )
        return c

    lax.fori_loop(1, n, one, 0)
    pl.semaphore_wait(barrier, n - 1)


def split(a):
    high = a.astype(BF16).astype(F32)
    rest = a - high
    mid = rest.astype(BF16).astype(F32)
    return high, mid, rest - mid


def stack(parts, axis):
    return jnp.concatenate(parts, axis=axis).astype(BF16)


def dot(a, b, ca, cb):
    return lax.dot_general(a, b, (((ca,), (cb,)), ((), ())), preferred_element_type=F32)


def fold_rows(p):
    r = p.shape[0] // 3
    return p[:r] + (p[r : 2 * r] + p[2 * r :])


def fold_lanes(p):
    c = p.shape[1] // 3
    return p[:, :c] + (p[:, c : 2 * c] + p[:, 2 * c :])


def inverse_factors(grams):
    size = grams[0].shape[0]
    eye = (
        lax.broadcasted_iota(jnp.int32, (size, size), 0)
        == lax.broadcasted_iota(jnp.int32, (size, size), 1)
    ).astype(F32)
    rest = [jnp.concatenate([g, eye], axis=1) for g in grams]
    wide = 2 * size
    sub = lax.broadcasted_iota(jnp.int32, (8, wide), 0)
    lane = lax.broadcasted_iota(jnp.int32, (8, size), 1)
    done = [[] for _ in grams]
    for t in range(size // 8):
        tiles = [a[8 * t : 8 * t + 8] for a in rest]
        cols = [
            [jnp.broadcast_to(a[:, 8 * t + j : 8 * t + j + 1], (8, wide)) for j in range(8)]
            for a in tiles
        ]
        invs = [jnp.zeros((8, wide), F32) for _ in tiles]
        for j in range(8):
            for i in range(len(tiles)):
                c = cols[i]
                inv = 1.0 / c[j][j : j + 1]
                below = jnp.where(sub > j, c[j], 0.0)
                tiles[i] = tiles[i] - below * (tiles[i][j : j + 1] * inv)
                for k in range(j + 1, 8):
                    c[k] = c[k] - below * (c[k][j : j + 1] * inv)
                invs[i] = jnp.where(sub == j, inv, invs[i])
        for i in range(len(tiles)):
            done[i].append(tiles[i] * jnp.sqrt(invs[i]))
            if 8 * t + 8 < size:
                scaled = (tiles[i] * invs[i])[:, :size]
                h, m, l = split(jnp.where(lane >= 8 * t + 8, scaled, 0.0))
                rh, rm, rl = split(tiles[i])
                rest[i] = rest[i] - dot(
                    stack([l, h, m, m, h, h], 0), stack([rh, rl, rm, rh, rm, rh], 0), 0, 0
                )
    return [jnp.concatenate(d, axis=0)[:, size:] for d in done]


def collect_kernel(
    n, inner, data_ref, start_ref, steer_ref, basis_ref, noise_ref,
    x_v, start_v, steer_v, flat_v, s_v, v_v, basis_v, power_v,
    send_sem, recv_sem, own_sem, start_sem, steer_sem, basis_sem,
):
    nb, _, rows, m = x_v.shape
    kk = n * rows
    g = steer_ref.shape[2]
    group = flat_v.shape[0]
    groups = nb // group
    me = lax.axis_index("snap") * inner + lax.axis_index("bin")

    own = pltpu.make_async_copy(data_ref.at[pl.ds(me * nb, nb)], x_v.at[:, 0], own_sem)
    first = pltpu.make_async_copy(start_ref, start_v, start_sem)

    def load(b):
        return pltpu.make_async_copy(steer_ref.at[b], steer_v.at[b], steer_sem.at[b])

    def put(p):
        return pltpu.make_async_copy(
            basis_v.at[pl.ds(p * group, group)], basis_ref.at[pl.ds(p * group, group)], basis_sem.at[p]
        )

    own.start()
    first.start()

    def fetch(b, c):
        load(b).start()
        return c

    lax.fori_loop(0, nb, fetch, 0)
    greet_all(me, n, inner)

    def copy(p, o):
        d = lax.rem(me + o, n)
        return pltpu.make_async_remote_copy(
            src_ref=data_ref.at[pl.ds(d * nb + p * group, group)],
            dst_ref=x_v.at[pl.ds(p * group, group), o],
            send_sem=send_sem.at[p],
            recv_sem=recv_sem.at[p],
            device_id=place(d, inner),
            device_id_type=MESH,
        )

    def post(p, c):
        def one(o, cc):
            copy(p, o).start()
            return cc

        return lax.fori_loop(1, n, one, c)

    lax.fori_loop(0, groups, post, 0)

    def arrived(p, sem):
        block = x_v.at[pl.ds(p * group, group), pl.ds(1, n - 1)]
        pltpu.make_async_copy(block, block, sem.at[p]).wait()

    power_v[...] = jnp.zeros_like(power_v)
    lanes = g // 4

    def energies(b, c):
        load(b).wait()
        for q in range(0, g, lanes):
            energy = power_v[:, q : q + lanes]
            for r in range(0, m, 64):
                part = steer_v[b, r : r + 64, q : q + lanes].astype(F32)
                energy = energy + jnp.sum((part * part).reshape(8, 8, lanes), axis=0)
            power_v[:, q : q + lanes] = energy
        return c

    lax.fori_loop(0, nb, energies, 0)
    noise_ref[...] = jnp.sum(power_v[...], axis=0, keepdims=True)
    own.wait()
    first.wait()

    def process(p, c):
        arrived(p, recv_sem)
        for i in range(group):
            b = p * group + i
            x = x_v[b].reshape(kk, m)
            flat_v[i] = x
            s_v[i] = stack(split(dot(x, x, 1, 1)), 1)
            v_v[i] = fold_rows(dot(stack(split(start_v[b]), 0), x, 1, 1))

        def step(it, cc):
            last = it == ITERS - 1
            kept, grams = [], []
            for i in range(group):
                v = v_v[i]
                vs = stack(split(v), 0)
                w = fold_rows(fold_lanes(dot(vs, s_v[i], 1, 0)))
                grams.append(fold_lanes(fold_rows(dot(stack(split(w), 0), vs, 1, 1))))
                kept.append(jnp.where(last, v, w * (1.0 / kk)))
            for i, factor in enumerate(inverse_factors(grams)):
                q = dot(stack(split(factor), 0), stack(split(kept[i]), 1), 1, 0)
                v_v[i] = fold_rows(fold_lanes(q))
            return cc

        lax.fori_loop(0, ITERS, step, 0)
        for i in range(group):
            b = p * group + i
            basis = fold_rows(dot(stack(split(v_v[i]), 0), flat_v[i], 1, 0))
            low = basis.astype(BF16)
            basis_v[b, 0] = low
            basis_v[b, 1] = (basis - low.astype(F32)).astype(BF16)
            for q in range(0, g, lanes):
                along = dot(low, steer_v[b, :, q : q + lanes], 1, 0)
                noise_ref[:, q : q + lanes] -= jnp.sum(along * along, axis=0, keepdims=True)
        put(p).start()
        return c

    lax.fori_loop(0, groups, process, 0)

    def close(p, c):
        arrived(p, send_sem)
        put(p).wait()
        return c

    lax.fori_loop(0, groups, close, 0)


def collect(data, start, steering, n, inner):
    bins, rows, m = data.shape
    nb = bins // n
    kk = n * rows
    width = start.shape[1]
    g = steering.shape[2]
    group = 2 if nb % 2 == 0 else 1
    groups = nb // group
    return pl.pallas_call(
        functools.partial(collect_kernel, n, inner),
        out_shape=(
            jax.ShapeDtypeStruct((nb, 2, width, m), BF16),
            jax.ShapeDtypeStruct((1, g), F32),
        ),
        in_specs=[pl.BlockSpec(memory_space=pl.ANY)] * 3,
        out_specs=(
            pl.BlockSpec(memory_space=pl.ANY),
            pl.BlockSpec(memory_space=pltpu.VMEM),
        ),
        scratch_shapes=[
            pltpu.VMEM((nb, n, rows, m), BF16),
            pltpu.VMEM((nb, width, m), F32),
            pltpu.VMEM((nb, m, g), BF16),
            pltpu.VMEM((group, kk, m), BF16),
            pltpu.VMEM((group, kk, 3 * kk), BF16),
            pltpu.VMEM((group, width, kk), F32),
            pltpu.VMEM((nb, 2, width, m), BF16),
            pltpu.VMEM((8, g), F32),
            pltpu.SemaphoreType.DMA((groups,)),
            pltpu.SemaphoreType.DMA((groups,)),
            pltpu.SemaphoreType.DMA,
            pltpu.SemaphoreType.DMA,
            pltpu.SemaphoreType.DMA((nb,)),
            pltpu.SemaphoreType.DMA((groups,)),
        ],
        compiler_params=pltpu.CompilerParams(
            collective_id=0, has_side_effects=True, vmem_limit_bytes=VMEM_LIMIT
        ),
        name="collect",
    )(data, start, steering)


SLOTS = 8


def project_kernel(basis_ref, proj_ref, basis_v, out_v, in_sem, out_sem):
    nb, _, width, m = basis_ref.shape
    step_rows = out_v.shape[1]
    per = m // step_rows

    def load(b):
        return pltpu.make_async_copy(basis_ref.at[b], basis_v.at[b], in_sem.at[b])

    def put(b, r):
        slot = lax.rem(b * per + r, SLOTS)
        return pltpu.make_async_copy(
            out_v.at[slot], proj_ref.at[b, pl.ds(r * step_rows, step_rows)], out_sem.at[slot]
        )

    def fetch(b, c):
        load(b).start()
        return c

    lax.fori_loop(0, nb, fetch, 0)

    def one(b, c):
        load(b).wait()
        low = basis_v[b, 0]
        tail = basis_v[b, 1]
        left = jnp.concatenate([low, tail, low], axis=0)
        right = jnp.concatenate([low, low, tail], axis=0)
        for r in range(per):

            @pl.when(b * per + r >= SLOTS)
            def _():
                put(b, r).wait()

            slot = lax.rem(b * per + r, SLOTS)
            out_v[slot] = dot(left[:, r * step_rows : (r + 1) * step_rows], right, 0, 0)
            put(b, r).start()
        return c

    lax.fori_loop(0, nb, one, 0)

    def drain(t, c):
        put(t // per, lax.rem(t, per)).wait()
        return c

    lax.fori_loop(max(nb * per - SLOTS, 0), nb * per, drain, 0)


def project(basis):
    nb, _, width, m = basis.shape
    step_rows = m // 4
    return pl.pallas_call(
        project_kernel,
        out_shape=jax.ShapeDtypeStruct((nb, m, m), F32),
        in_specs=[pl.BlockSpec(memory_space=pl.ANY)],
        out_specs=pl.BlockSpec(memory_space=pl.ANY),
        scratch_shapes=[
            pltpu.VMEM((nb, 2, width, m), BF16),
            pltpu.VMEM((SLOTS, step_rows, m), F32),
            pltpu.SemaphoreType.DMA((nb,)),
            pltpu.SemaphoreType.DMA((SLOTS,)),
        ],
        compiler_params=pltpu.CompilerParams(vmem_limit_bytes=VMEM_LIMIT),
        cost_estimate=pl.CostEstimate(
            flops=nb * m * m * width * 6, bytes_accessed=nb * m * m * 4, transcendentals=0
        ),
        name="project",
    )(basis)


def on_device(n, inner, data, steering, start):
    bins, rows, m = data.shape
    basis, noise = collect(data, start.transpose(0, 2, 1), steering, n, inner)
    held = lax.all_to_all(jnp.broadcast_to(noise, (n, noise.shape[1])), BOTH, 0, 0)
    projector = project(basis)
    spectrum = float(bins * m) / jnp.sum(held, axis=0)
    return (projector, spectrum)


def solution(mesh):
    P = jax.sharding.PartitionSpec
    inner = mesh.shape["bin"]
    n = mesh.shape["snap"] * inner
    return jax.shard_map(
        functools.partial(on_device, n, inner),
        mesh=mesh,
        in_specs=(P(None, BOTH, None), P(BOTH, None, None), P(BOTH, None, None)),
        out_specs=(P(BOTH, None, None), P()),
        check_vma=False,
    )
```

```python
import functools

import jax
import jax.numpy as jnp
from jax import lax
from jax.experimental import pallas as pl
from jax.experimental.pallas import tpu as pltpu

ITERS = 3
PIVOTS = 16
F32 = jnp.float32
BF16 = jnp.bfloat16
MESH = pl.DeviceIdType.MESH
VMEM_LIMIT = 60 * 1024 * 1024
BOTH = ("snap", "bin")


def place(d, inner):
    return (d // inner, lax.rem(d, inner))


def greet_all(me, n, inner):
    barrier = pltpu.get_barrier_semaphore()

    def one(o, c):
        pl.semaphore_signal(
            barrier, inc=1, device_id=place(lax.rem(me + o, n), inner), device_id_type=MESH
        )
        return c

    lax.fori_loop(1, n, one, 0)
    pl.semaphore_wait(barrier, n - 1)


def split(a):
    high = a.astype(BF16).astype(F32)
    rest = a - high
    mid = rest.astype(BF16).astype(F32)
    return high, mid, rest - mid


def stack(parts, axis):
    return jnp.concatenate(parts, axis=axis).astype(BF16)


def dot(a, b, ca, cb):
    return lax.dot_general(a, b, (((ca,), (cb,)), ((), ())), preferred_element_type=F32)


def fold_rows(p):
    r = p.shape[0] // 3
    return p[:r] + (p[r : 2 * r] + p[2 * r :])


def fold_lanes(p):
    c = p.shape[1] // 3
    return p[:, :c] + (p[:, c : 2 * c] + p[:, 2 * c :])


def inverse_factors(ga, gb):
    size = ga.shape[0]
    wide = 2 * size
    shape = (size, wide)
    col = lax.broadcasted_iota(jnp.int32, shape, 1)
    col = jnp.where(col >= size, col - size, col)
    both = jnp.concatenate([ga, gb], axis=1)
    unit = (col == lax.broadcasted_iota(jnp.int32, shape, 0)).astype(F32)
    sub = lax.broadcasted_iota(jnp.int32, (PIVOTS, wide), 0)
    lane = lax.broadcasted_iota(jnp.int32, (PIVOTS, wide), 1)
    first = lane < size
    lane = jnp.where(first, lane, lane - size)
    pick = lax.broadcasted_iota(jnp.int32, (size, 2 * wide), 1)
    pick = jnp.where(pick >= wide, pick - wide, pick) < size
    done = []
    for t in range(0, size, PIVOTS):
        g = both[t : t + PIVOTS]
        u = unit[t : t + PIVOTS]
        c = [
            jnp.where(
                first,
                jnp.broadcast_to(g[:, k : k + 1], (PIVOTS, wide)),
                jnp.broadcast_to(g[:, size + k : size + k + 1], (PIVOTS, wide)),
            )
            for k in range(t, t + PIVOTS)
        ]
        invs = jnp.zeros((PIVOTS, wide), F32)
        for j in range(PIVOTS):
            inv = 1.0 / c[j][j : j + 1]
            below = jnp.where(sub > j, c[j], 0.0)
            g = g - below * (g[j : j + 1] * inv)
            u = u - below * (u[j : j + 1] * inv)
            for k in range(j + 1, PIVOTS):
                c[k] = c[k] - below * (c[k][j : j + 1] * inv)
            invs = jnp.where(sub == j, inv, invs)
        done.append(u * jnp.sqrt(invs))
        if t + PIVOTS < size:
            h, m, l = split(jnp.where(lane >= t + PIVOTS, g * invs, 0.0))
            rh, rm, rl = split(jnp.concatenate([g, u], axis=1))
            d = dot(stack([l, h, m, m, h, h], 0), stack([rh, rl, rm, rh, rm, rh], 0), 0, 0)
            d = jnp.where(pick, d[:size], d[size:])
            both = both - d[:, :wide]
            unit = unit - d[:, wide:]
    f = jnp.concatenate(done, axis=0)
    return f[:, :size], f[:, size:]


def collect_kernel(
    n, inner, data_ref, start_ref, steer_ref, basis_ref, noise_ref,
    x_v, start_v, steer_v, flat_v, s_v, v_v, basis_v, power_v, total_v,
    send_sem, recv_sem, own_sem, start_sem, steer_sem, basis_sem,
):
    nb, _, rows, m = x_v.shape
    kk = n * rows
    g = steer_ref.shape[2]
    group = flat_v.shape[0]
    groups = nb // group
    me = lax.axis_index("snap") * inner + lax.axis_index("bin")

    own = pltpu.make_async_copy(data_ref.at[pl.ds(me * nb, nb)], x_v.at[:, 0], own_sem)
    first = pltpu.make_async_copy(start_ref, start_v, start_sem)

    def load(b):
        return pltpu.make_async_copy(steer_ref.at[b], steer_v.at[b], steer_sem.at[b])

    def put(p):
        return pltpu.make_async_copy(
            basis_v.at[pl.ds(p * group, group)], basis_ref.at[pl.ds(p * group, group)], basis_sem.at[p]
        )

    own.start()
    first.start()

    def fetch(b, c):
        load(b).start()
        return c

    lax.fori_loop(0, nb, fetch, 0)
    greet_all(me, n, inner)

    def copy(p, o):
        d = lax.rem(me + o, n)
        return pltpu.make_async_remote_copy(
            src_ref=data_ref.at[pl.ds(d * nb + p * group, group)],
            dst_ref=x_v.at[pl.ds(p * group, group), o],
            send_sem=send_sem.at[p],
            recv_sem=recv_sem.at[p],
            device_id=place(d, inner),
            device_id_type=MESH,
        )

    def post(p, c):
        def one(o, cc):
            copy(p, o).start()
            return cc

        return lax.fori_loop(1, n, one, c)

    lead = min(2, groups)
    lax.fori_loop(0, lead, post, 0)

    def arrived(p, sem):
        block = x_v.at[pl.ds(p * group, group), pl.ds(1, n - 1)]
        pltpu.make_async_copy(block, block, sem.at[p]).wait()

    power_v[...] = jnp.zeros_like(power_v)
    lanes = g // 4

    def energies(b, c):
        load(b).wait()
        for q in range(0, g, lanes):
            energy = power_v[:, q : q + lanes]
            for r in range(0, m, 64):
                part = steer_v[b, r : r + 64, q : q + lanes].astype(F32)
                energy = energy + jnp.sum((part * part).reshape(8, 8, lanes), axis=0)
            power_v[:, q : q + lanes] = energy
        return c

    lax.fori_loop(0, nb, energies, 0)
    total_v[...] = jnp.sum(power_v[...], axis=0, keepdims=True)
    own.wait()
    first.wait()

    def process(p, c):
        arrived(p, recv_sem)

        @pl.when(p + lead < groups)
        def _():
            post(p + lead, 0)

        for i in range(group):
            b = p * group + i
            x = x_v[b].reshape(kk, m)
            flat_v[i] = x
            s_v[i] = stack(split(dot(x, x, 1, 1)), 1)
            v_v[i] = fold_rows(dot(stack(split(start_v[b]), 0), x, 1, 1))

        def step(it, cc):
            last = it == ITERS - 1
            kept, grams = [], []
            for i in range(group):
                v = v_v[i]
                vs = stack(split(v), 0)
                w = fold_rows(fold_lanes(dot(vs, s_v[i], 1, 0)))
                grams.append(fold_lanes(fold_rows(dot(stack(split(w), 0), vs, 1, 1))))
                kept.append(jnp.where(last, v, w * (1.0 / kk)))
            for i, factor in zip(range(group), inverse_factors(grams[0], grams[-1])):
                q = dot(stack(split(factor), 0), stack(split(kept[i]), 1), 1, 0)
                v_v[i] = fold_rows(fold_lanes(q))
            return cc

        lax.fori_loop(0, ITERS, step, 0)
        for i in range(group):
            b = p * group + i
            basis = fold_rows(dot(stack(split(v_v[i]), 0), flat_v[i], 1, 0))
            low = basis.astype(BF16)
            basis_v[b, 0] = low
            basis_v[b, 1] = (basis - low.astype(F32)).astype(BF16)
            for q in range(0, g, lanes):
                along = dot(low, steer_v[b, :, q : q + lanes], 1, 0)
                total_v[:, q : q + lanes] -= jnp.sum(along * along, axis=0, keepdims=True)
        put(p).start()
        return c

    lax.fori_loop(0, groups, process, 0)
    noise_ref[...] = jnp.broadcast_to(total_v[...][None], noise_ref.shape)

    def close(p, c):
        arrived(p, send_sem)
        put(p).wait()
        return c

    lax.fori_loop(0, groups, close, 0)


def collect(data, start, steering, n, inner):
    bins, rows, m = data.shape
    nb = bins // n
    kk = n * rows
    width = start.shape[1]
    g = steering.shape[2]
    group = 2 if nb % 2 == 0 else 1
    groups = nb // group
    return pl.pallas_call(
        functools.partial(collect_kernel, n, inner),
        out_shape=(
            jax.ShapeDtypeStruct((nb, 2, width, m), BF16),
            jax.ShapeDtypeStruct((n, 1, g), F32),
        ),
        in_specs=[pl.BlockSpec(memory_space=pl.ANY)] * 3,
        out_specs=(
            pl.BlockSpec(memory_space=pl.ANY),
            pl.BlockSpec(memory_space=pltpu.VMEM),
        ),
        scratch_shapes=[
            pltpu.VMEM((nb, n, rows, m), BF16),
            pltpu.VMEM((nb, width, m), F32),
            pltpu.VMEM((nb, m, g), BF16),
            pltpu.VMEM((group, kk, m), BF16),
            pltpu.VMEM((group, kk, 3 * kk), BF16),
            pltpu.VMEM((group, width, kk), F32),
            pltpu.VMEM((nb, 2, width, m), BF16),
            pltpu.VMEM((8, g), F32),
            pltpu.VMEM((1, g), F32),
            pltpu.SemaphoreType.DMA((groups,)),
            pltpu.SemaphoreType.DMA((groups,)),
            pltpu.SemaphoreType.DMA,
            pltpu.SemaphoreType.DMA,
            pltpu.SemaphoreType.DMA((nb,)),
            pltpu.SemaphoreType.DMA((groups,)),
        ],
        compiler_params=pltpu.CompilerParams(
            collective_id=0, has_side_effects=True, vmem_limit_bytes=VMEM_LIMIT
        ),
        name="collect",
    )(data, start, steering)


SLOTS = 8


def project_kernel(basis_ref, proj_ref, basis_v, out_v, in_sem, out_sem):
    nb, _, width, m = basis_ref.shape
    step_rows = out_v.shape[1]
    per = m // step_rows

    def load(b):
        return pltpu.make_async_copy(basis_ref.at[b], basis_v.at[b], in_sem.at[b])

    def put(b, r):
        slot = lax.rem(b * per + r, SLOTS)
        return pltpu.make_async_copy(
            out_v.at[slot], proj_ref.at[b, pl.ds(r * step_rows, step_rows)], out_sem.at[slot]
        )

    def fetch(b, c):
        load(b).start()
        return c

    lax.fori_loop(0, nb, fetch, 0)

    def one(b, c):
        load(b).wait()
        low = basis_v[b, 0]
        tail = basis_v[b, 1]
        left = jnp.concatenate([low, tail, low], axis=0)
        right = jnp.concatenate([low, low, tail], axis=0)
        for r in range(per):

            @pl.when(b * per + r >= SLOTS)
            def _():
                put(b, r).wait()

            slot = lax.rem(b * per + r, SLOTS)
            out_v[slot] = dot(left[:, r * step_rows : (r + 1) * step_rows], right, 0, 0)
            put(b, r).start()
        return c

    lax.fori_loop(0, nb, one, 0)

    def drain(t, c):
        put(t // per, lax.rem(t, per)).wait()
        return c

    lax.fori_loop(max(nb * per - SLOTS, 0), nb * per, drain, 0)


def project(basis):
    nb, _, width, m = basis.shape
    step_rows = m // 4
    return pl.pallas_call(
        project_kernel,
        out_shape=jax.ShapeDtypeStruct((nb, m, m), F32),
        in_specs=[pl.BlockSpec(memory_space=pl.ANY)],
        out_specs=pl.BlockSpec(memory_space=pl.ANY),
        scratch_shapes=[
            pltpu.VMEM((nb, 2, width, m), BF16),
            pltpu.VMEM((SLOTS, step_rows, m), F32),
            pltpu.SemaphoreType.DMA((nb,)),
            pltpu.SemaphoreType.DMA((SLOTS,)),
        ],
        compiler_params=pltpu.CompilerParams(vmem_limit_bytes=VMEM_LIMIT),
        cost_estimate=pl.CostEstimate(
            flops=nb * m * m * width * 6, bytes_accessed=nb * m * m * 4, transcendentals=0
        ),
        name="project",
    )(basis)


def on_device(n, inner, data, steering, start):
    bins, rows, m = data.shape
    basis, noise = collect(data, start.transpose(0, 2, 1), steering, n, inner)
    held = lax.all_to_all(noise, BOTH, 0, 0)
    projector = project(basis)
    spectrum = float(bins * m) / jnp.sum(held, axis=(0, 1))
    return (projector, spectrum)


def solution(mesh):
    P = jax.sharding.PartitionSpec
    inner = mesh.shape["bin"]
    n = mesh.shape["snap"] * inner
    return jax.shard_map(
        functools.partial(on_device, n, inner),
        mesh=mesh,
        in_specs=(P(None, BOTH, None), P(BOTH, None, None), P(BOTH, None, None)),
        out_specs=(P(BOTH, None, None), P()),
        check_vma=False,
    )
```

```python
import functools

import jax
import jax.numpy as jnp
from jax import lax
from jax.experimental import pallas as pl
from jax.experimental.pallas import tpu as pltpu

ITERS = 3
PIVOTS = 16
F32 = jnp.float32
BF16 = jnp.bfloat16
MESH = pl.DeviceIdType.MESH
VMEM_LIMIT = 60 * 1024 * 1024
BOTH = ("snap", "bin")


def place(d, inner):
    return (d // inner, lax.rem(d, inner))


def greet_all(me, n, inner):
    barrier = pltpu.get_barrier_semaphore()

    def one(o, c):
        pl.semaphore_signal(
            barrier, inc=1, device_id=place(lax.rem(me + o, n), inner), device_id_type=MESH
        )
        return c

    lax.fori_loop(1, n, one, 0)
    pl.semaphore_wait(barrier, n - 1)


def split(a):
    high = a.astype(BF16).astype(F32)
    rest = a - high
    mid = rest.astype(BF16).astype(F32)
    return high, mid, rest - mid


def stack(parts, axis):
    return jnp.concatenate(parts, axis=axis).astype(BF16)


def dot(a, b, ca, cb):
    return lax.dot_general(a, b, (((ca,), (cb,)), ((), ())), preferred_element_type=F32)


def fold_rows(p):
    r = p.shape[0] // 3
    return p[:r] + (p[r : 2 * r] + p[2 * r :])


def fold_lanes(p):
    c = p.shape[1] // 3
    return p[:, :c] + (p[:, c : 2 * c] + p[:, 2 * c :])


def inverse_factors(ga, gb):
    size = ga.shape[0]
    wide = 2 * size
    shape = (size, wide)
    col = lax.broadcasted_iota(jnp.int32, shape, 1)
    col = jnp.where(col >= size, col - size, col)
    both = jnp.concatenate([ga, gb], axis=1)
    unit = (col == lax.broadcasted_iota(jnp.int32, shape, 0)).astype(F32)
    sub = lax.broadcasted_iota(jnp.int32, (PIVOTS, wide), 0)
    lane = lax.broadcasted_iota(jnp.int32, (PIVOTS, wide), 1)
    first = lane < size
    lane = jnp.where(first, lane, lane - size)
    pick = lax.broadcasted_iota(jnp.int32, (size, 2 * wide), 1)
    pick = jnp.where(pick >= wide, pick - wide, pick) < size
    done = []
    for t in range(0, size, PIVOTS):
        g = both[t : t + PIVOTS]
        u = unit[t : t + PIVOTS]
        c = [
            jnp.where(
                first,
                jnp.broadcast_to(g[:, k : k + 1], (PIVOTS, wide)),
                jnp.broadcast_to(g[:, size + k : size + k + 1], (PIVOTS, wide)),
            )
            for k in range(t, t + PIVOTS)
        ]
        invs = jnp.zeros((PIVOTS, wide), F32)
        for j in range(PIVOTS):
            inv = 1.0 / c[j][j : j + 1]
            below = jnp.where(sub > j, c[j], 0.0)
            g = g - below * (g[j : j + 1] * inv)
            u = u - below * (u[j : j + 1] * inv)
            for k in range(j + 1, PIVOTS):
                c[k] = c[k] - below * (c[k][j : j + 1] * inv)
            invs = jnp.where(sub == j, inv, invs)
        done.append(u * jnp.sqrt(invs))
        if t + PIVOTS < size:
            h, m, l = split(jnp.where(lane >= t + PIVOTS, g * invs, 0.0))
            rh, rm, rl = split(jnp.concatenate([g, u], axis=1))
            d = dot(stack([l, h, m, m, h, h], 0), stack([rh, rl, rm, rh, rm, rh], 0), 0, 0)
            d = jnp.where(pick, d[:size], d[size:])
            both = both - d[:, :wide]
            unit = unit - d[:, wide:]
    f = jnp.concatenate(done, axis=0)
    return f[:, :size], f[:, size:]


def collect_kernel(
    n, inner, data_ref, start_ref, steer_ref, basis_ref, noise_ref,
    x_v, start_v, steer_v, flat_v, s_v, v_v, basis_v, power_v, total_v, parts_v,
    send_sem, recv_sem, own_sem, start_sem, steer_sem, basis_sem,
):
    nb, _, rows, m = x_v.shape
    kk = n * rows
    g = steer_ref.shape[2]
    group = flat_v.shape[0]
    groups = nb // group
    me = lax.axis_index("snap") * inner + lax.axis_index("bin")

    own = pltpu.make_async_copy(data_ref.at[pl.ds(me * nb, nb)], x_v.at[:, 0], own_sem)
    first = pltpu.make_async_copy(start_ref, start_v, start_sem)

    def load(b):
        return pltpu.make_async_copy(steer_ref.at[b], steer_v.at[b], steer_sem.at[b])

    def put(p):
        return pltpu.make_async_copy(
            basis_v.at[pl.ds(p * group, group)], basis_ref.at[pl.ds(p * group, group)], basis_sem.at[p]
        )

    own.start()
    first.start()

    def fetch(b, c):
        load(b).start()
        return c

    lax.fori_loop(0, nb, fetch, 0)
    greet_all(me, n, inner)

    def copy(p, o):
        d = lax.rem(me + o, n)
        return pltpu.make_async_remote_copy(
            src_ref=data_ref.at[pl.ds(d * nb + p * group, group)],
            dst_ref=x_v.at[pl.ds(p * group, group), o],
            send_sem=send_sem.at[p],
            recv_sem=recv_sem.at[p],
            device_id=place(d, inner),
            device_id_type=MESH,
        )

    def post(p, c):
        def one(o, cc):
            copy(p, o).start()
            return cc

        return lax.fori_loop(1, n, one, c)

    lead = min(2, groups)
    lax.fori_loop(0, lead, post, 0)

    def arrived(p, sem):
        block = x_v.at[pl.ds(p * group, group), pl.ds(1, n - 1)]
        pltpu.make_async_copy(block, block, sem.at[p]).wait()

    power_v[...] = jnp.zeros_like(power_v)
    lanes = g // 4

    def energies(b, c):
        load(b).wait()
        for q in range(0, g, lanes):
            energy = power_v[:, q : q + lanes]
            for r in range(0, m, 64):
                part = steer_v[b, r : r + 64, q : q + lanes].astype(F32)
                energy = energy + jnp.sum((part * part).reshape(8, 8, lanes), axis=0)
            power_v[:, q : q + lanes] = energy
        return c

    lax.fori_loop(0, nb, energies, 0)
    total_v[...] = jnp.sum(power_v[...], axis=0, keepdims=True)
    own.wait()
    first.wait()

    def cut(b, c):
        parts_v[b] = stack(split(start_v[b]), 0)
        return c

    lax.fori_loop(0, nb, cut, 0)

    def process(p, c):
        arrived(p, recv_sem)

        @pl.when(p + lead < groups)
        def _():
            post(p + lead, 0)

        for i in range(group):
            b = p * group + i
            x = x_v[b].reshape(kk, m)
            flat_v[i] = x
            s_v[i] = stack(split(dot(x, x, 1, 1)), 1)
            v_v[i] = fold_rows(dot(parts_v[b], x, 1, 1))

        def step(it, cc):
            last = it == ITERS - 1
            kept, grams = [], []
            for i in range(group):
                v = v_v[i]
                vs = stack(split(v), 0)
                w = fold_rows(fold_lanes(dot(vs, s_v[i], 1, 0)))
                grams.append(fold_lanes(fold_rows(dot(stack(split(w), 0), vs, 1, 1))))
                kept.append(jnp.where(last, v, w * (1.0 / kk)))
            for i, factor in zip(range(group), inverse_factors(grams[0], grams[-1])):
                q = dot(stack(split(factor), 0), stack(split(kept[i]), 1), 1, 0)
                v_v[i] = fold_rows(fold_lanes(q))
            return cc

        lax.fori_loop(0, ITERS, step, 0)
        for i in range(group):
            b = p * group + i
            basis = fold_rows(dot(stack(split(v_v[i]), 0), flat_v[i], 1, 0))
            low = basis.astype(BF16)
            basis_v[b, 0] = low
            basis_v[b, 1] = (basis - low.astype(F32)).astype(BF16)
            for q in range(0, g, lanes):
                along = dot(low, steer_v[b, :, q : q + lanes], 1, 0)
                total_v[:, q : q + lanes] -= jnp.sum(along * along, axis=0, keepdims=True)
        put(p).start()
        return c

    lax.fori_loop(0, groups, process, 0)
    noise_ref[...] = jnp.broadcast_to(total_v[...][None], noise_ref.shape)

    def close(p, c):
        arrived(p, send_sem)
        put(p).wait()
        return c

    lax.fori_loop(0, groups, close, 0)


def collect(data, start, steering, n, inner):
    bins, rows, m = data.shape
    nb = bins // n
    kk = n * rows
    width = start.shape[1]
    g = steering.shape[2]
    group = 2 if nb % 2 == 0 else 1
    groups = nb // group
    return pl.pallas_call(
        functools.partial(collect_kernel, n, inner),
        out_shape=(
            jax.ShapeDtypeStruct((nb, 2, width, m), BF16),
            jax.ShapeDtypeStruct((n, 1, g), F32),
        ),
        in_specs=[pl.BlockSpec(memory_space=pl.ANY)] * 3,
        out_specs=(
            pl.BlockSpec(memory_space=pl.ANY),
            pl.BlockSpec(memory_space=pltpu.VMEM),
        ),
        scratch_shapes=[
            pltpu.VMEM((nb, n, rows, m), BF16),
            pltpu.VMEM((nb, width, m), F32),
            pltpu.VMEM((nb, m, g), BF16),
            pltpu.VMEM((group, kk, m), BF16),
            pltpu.VMEM((group, kk, 3 * kk), BF16),
            pltpu.VMEM((group, width, kk), F32),
            pltpu.VMEM((nb, 2, width, m), BF16),
            pltpu.VMEM((8, g), F32),
            pltpu.VMEM((1, g), F32),
            pltpu.VMEM((nb, 3 * width, m), BF16),
            pltpu.SemaphoreType.DMA((groups,)),
            pltpu.SemaphoreType.DMA((groups,)),
            pltpu.SemaphoreType.DMA,
            pltpu.SemaphoreType.DMA,
            pltpu.SemaphoreType.DMA((nb,)),
            pltpu.SemaphoreType.DMA((groups,)),
        ],
        compiler_params=pltpu.CompilerParams(
            collective_id=0, has_side_effects=True, vmem_limit_bytes=VMEM_LIMIT
        ),
        name="collect",
    )(data, start, steering)


SLOTS = 8


def project_kernel(basis_ref, proj_ref, basis_v, out_v, in_sem, out_sem):
    nb, _, width, m = basis_ref.shape
    step_rows = out_v.shape[1]
    per = m // step_rows

    def load(b):
        return pltpu.make_async_copy(basis_ref.at[b], basis_v.at[b], in_sem.at[b])

    def put(b, r):
        slot = lax.rem(b * per + r, SLOTS)
        return pltpu.make_async_copy(
            out_v.at[slot], proj_ref.at[b, pl.ds(r * step_rows, step_rows)], out_sem.at[slot]
        )

    def fetch(b, c):
        load(b).start()
        return c

    lax.fori_loop(0, nb, fetch, 0)

    def one(b, c):
        load(b).wait()
        low = basis_v[b, 0]
        tail = basis_v[b, 1]
        left = jnp.concatenate([low, tail, low], axis=0)
        right = jnp.concatenate([low, low, tail], axis=0)
        for r in range(per):

            @pl.when(b * per + r >= SLOTS)
            def _():
                put(b, r).wait()

            slot = lax.rem(b * per + r, SLOTS)
            out_v[slot] = dot(left[:, r * step_rows : (r + 1) * step_rows], right, 0, 0)
            put(b, r).start()
        return c

    lax.fori_loop(0, nb, one, 0)

    def drain(t, c):
        put(t // per, lax.rem(t, per)).wait()
        return c

    lax.fori_loop(max(nb * per - SLOTS, 0), nb * per, drain, 0)


def project(basis):
    nb, _, width, m = basis.shape
    step_rows = m // 4
    return pl.pallas_call(
        project_kernel,
        out_shape=jax.ShapeDtypeStruct((nb, m, m), F32),
        in_specs=[pl.BlockSpec(memory_space=pl.ANY)],
        out_specs=pl.BlockSpec(memory_space=pl.ANY),
        scratch_shapes=[
            pltpu.VMEM((nb, 2, width, m), BF16),
            pltpu.VMEM((SLOTS, step_rows, m), F32),
            pltpu.SemaphoreType.DMA((nb,)),
            pltpu.SemaphoreType.DMA((SLOTS,)),
        ],
        compiler_params=pltpu.CompilerParams(vmem_limit_bytes=VMEM_LIMIT),
        cost_estimate=pl.CostEstimate(
            flops=nb * m * m * width * 6, bytes_accessed=nb * m * m * 4, transcendentals=0
        ),
        name="project",
    )(basis)


def on_device(n, inner, data, steering, start):
    bins, rows, m = data.shape
    basis, noise = collect(data, start.transpose(0, 2, 1), steering, n, inner)
    held = lax.all_to_all(noise, BOTH, 0, 0)
    projector = project(basis)
    spectrum = float(bins * m) / jnp.sum(held, axis=(0, 1))
    return (projector, spectrum)


def solution(mesh):
    P = jax.sharding.PartitionSpec
    inner = mesh.shape["bin"]
    n = mesh.shape["snap"] * inner
    return jax.shard_map(
        functools.partial(on_device, n, inner),
        mesh=mesh,
        in_specs=(P(None, BOTH, None), P(BOTH, None, None), P(BOTH, None, None)),
        out_specs=(P(BOTH, None, None), P()),
        check_vma=False,
    )
```
